32 devices in a mesh: rows: 8 (over y, x, core), cols: 4 (over z).
Axes of the slice: x: 2, y: 2, z: 4, core: 2. Of those that a mesh axis runs over, the one named last changes fastest.
Arguments:
- density: bfloat16 [640, 640], P('rows', 'cols'), as said below
- occupancy: int32 [5, 5], replicated, may hold values from 0 to 1, as said below
- square_filter: int32 [5, 5], replicated, may hold values 0 or 1
- cube_filter: int32 [5, 5], replicated, may hold values 0 or 1
Outputs:
- purified: float32 [640, 640], P('rows', 'cols')
The draws below stay inside these ranges and needn't reach their ends.
Inputs may be any that keep to these rules, and one draw needn't show every extreme that they name: density is symmetric. occupancy is symmetric and every diagonal tile is stored.
All inputs are finite; a program needn't handle non-finite values.
Results may differ from the reference program's by a relative error of at most 0.0095.
Values may be sent and summed in bfloat16 or wider, within the bound.
No kernel may reach another device: no remote copies, remote signals or barrier semaphores. Data moves between devices by JAX's collectives and lax.ppermute only.
A program may use at most 64 MiB of HBM per device.

```python
import jax
import jax.numpy as jnp
from jax import lax

TILE = 128
N = 640
NT = 5


def draw_density(key, part):
    first = jax.random.fold_in(key, 0)
    base = jax.random.normal(first, (N, N), jnp.float32)
    symmetric = (base + base.T) * 0.5 ** 0.5 / (0.4 * N) ** 0.5
    return symmetric.astype(jnp.bfloat16)


def draw_occupancy(key, part):
    draws = jax.random.randint(key, (NT, NT), 0, 1000)
    summed = draws + draws.T
    indices = jnp.arange(NT)
    gap = jnp.abs(indices[:, None] - indices[None, :])
    distance = jnp.minimum(gap, NT - gap)
    halfway = max(NT // 2, 1)
    limit = 1600 - 1200 * distance // halfway
    stored = (summed < limit) | (gap == 0)
    return stored.astype(jnp.int32)


def place_ends(array, own_key, smallest, largest):
    spot = [jax.random.randint(jax.random.fold_in(own_key, axis), (), 0, length) for axis, length in enumerate(array.shape)]
    longest = array.shape.index(max(array.shape))
    next_to = spot[:longest] + [(spot[longest] + 1) % array.shape[longest]] + spot[longest + 1:]
    return array.at[tuple(spot)].set(smallest).at[tuple(next_to)].set(largest)


def setup_inputs(seed: int = 0) -> dict:
    keys = jax.random.split(jax.random.key(seed), 5)
    return {
        "density": draw_density(jax.random.fold_in(keys[4], 71), 0),
        "occupancy": draw_occupancy(jax.random.fold_in(keys[4], 71), 0),
        "square_filter": place_ends((jax.random.randint(keys[2], (NT, NT), 0, 4) < 3).astype(jnp.int32), jax.random.fold_in(keys[2], 1), 0, 1),
        "cube_filter": place_ends((jax.random.randint(keys[3], (NT, NT), 0, 4) < 3).astype(jnp.int32), jax.random.fold_in(keys[3], 1), 0, 1),
    }


def expand(table):
    return jnp.repeat(jnp.repeat(table, TILE, axis=0), TILE, axis=1)


def reference(density, occupancy, square_filter, cube_filter):
    occupied = jnp.where(expand(occupancy) > 0, density, jnp.zeros_like(density))
    values = occupied.astype(jnp.float32)
    square_total = jnp.dot(values, values, precision=lax.Precision.HIGHEST)
    square = jnp.where(expand(square_filter) > 0, square_total, jnp.zeros_like(square_total)).astype(jnp.bfloat16)
    cube_total = jnp.dot(square.astype(jnp.float32), values, precision=lax.Precision.HIGHEST)
    cube = jnp.where(expand(cube_filter) > 0, cube_total, jnp.zeros_like(cube_total))
    return 3.0 * square.astype(jnp.float32) - 2.0 * cube
```

```python
import jax
import jax.numpy as jnp
from jax import lax
from jax.sharding import PartitionSpec as P

TILE = 128
SMALL = 4 * 1024 * 1024


def lookup(table, rows, cols):
    tiles = jnp.arange(table.shape[0], dtype=jnp.int32)
    row_pick = (rows[:, None] // TILE == tiles[None, :]).astype(jnp.bfloat16)
    col_pick = (tiles[:, None] == cols[None, :] // TILE).astype(jnp.bfloat16)
    left = jnp.dot(row_pick, table.astype(jnp.bfloat16))
    return jnp.dot(left, col_pick) > 0.5


def span(start, count):
    return jnp.arange(count, dtype=jnp.int32) + start


def gathered(density, occupancy, square_filter, cube_filter):
    b, w = density.shape
    rows = span(lax.axis_index("rows") * b, b)
    cols = span(lax.axis_index("cols") * w, w)
    occupied = jnp.where(lookup(occupancy, rows, cols), density, jnp.zeros_like(density))
    panel = lax.all_gather(occupied, "cols", axis=1, tiled=True)
    column = lax.all_gather(occupied, "rows", axis=0, tiled=True)
    total = jnp.dot(panel, column, preferred_element_type=jnp.float32)
    square = jnp.where(lookup(square_filter, rows, cols), total, 0.0).astype(jnp.bfloat16)
    square_rows = lax.all_gather(square, "cols", axis=1, tiled=True)
    cube = jnp.dot(square_rows, column, preferred_element_type=jnp.float32)
    cube = jnp.where(lookup(cube_filter, rows, cols), cube, 0.0)
    return 3.0 * square.astype(jnp.float32) - 2.0 * cube


def contract_last(a, b):
    return lax.dot_general(a, b, (((1,), (1,)), ((), ())), preferred_element_type=jnp.float32)


def permuted(density, occupancy, square_filter, cube_filter):
    b, w = density.shape
    n_rows, n_cols = lax.axis_size("rows"), lax.axis_size("cols")
    pairs = n_rows // 2
    r, j = lax.axis_index("rows"), lax.axis_index("cols")
    own, parity = r // 2, r % 2

    pieces = [density]
    for s in range(1, n_cols):
        pieces.append(lax.ppermute(density, "cols", [((d + s) % n_cols, d) for d in range(n_cols)]))
    order = jnp.concatenate([span((j + s) % n_cols * w, w) for s in range(n_cols)])
    rows = span(r * b, b)
    stored = lookup(occupancy, rows, order)
    panel = jnp.where(stored, jnp.concatenate(pieces, axis=1), jnp.zeros((), density.dtype))

    other = lax.ppermute(panel, "rows", [(d, d ^ 1) for d in range(n_rows)])
    shifts = sorted(range(1, pairs), key=lambda m: -m)
    panels, groups = [panel], [own]
    for m in shifts:
        panels.append(lax.ppermute(panel, "rows", [((d + 2 * m) % n_rows, d) for d in range(n_rows)]))
        groups.append((own + m) % pairs)
    kept = jnp.concatenate([span((2 * g + parity) * b, b) for g in groups])
    other_rows = span((r ^ 1) * b, b)
    pair_rows = jnp.concatenate([rows, other_rows])
    cols = span(j * w, w)
    square_mask = lookup(square_filter, pair_rows, kept)
    cube_mask = lookup(cube_filter, pair_rows, cols)
    pick = (kept[:, None] == cols[None, :]).astype(jnp.bfloat16)

    right = jnp.concatenate(panels, axis=0)
    left = jnp.concatenate([panel, other], axis=0)
    square = jnp.where(square_mask, contract_last(left, right), 0.0).astype(jnp.bfloat16)
    cube = jnp.dot(square, right[:, :w], preferred_element_type=jnp.float32)
    mine = jnp.dot(square, pick, preferred_element_type=jnp.float32)
    part = 3.0 * mine - 2.0 * jnp.where(cube_mask, cube, 0.0)
    return part[:b] + lax.ppermute(part[b:], "rows", [(d, d ^ 1) for d in range(n_rows)])


def solution(mesh):
    def on_device(density, *tables):
        n_rows, n_cols = mesh.shape["rows"], mesh.shape["cols"]
        small = density.size * n_rows * n_cols * density.dtype.itemsize <= SMALL
        body = permuted if small and n_rows % 2 == 0 else gathered
        return body(density, *tables)

    placed = (P("rows", "cols"), P(), P(), P())
    return jax.shard_map(
        on_device, mesh=mesh, in_specs=placed, out_specs=P("rows", "cols"), check_vma=False
    )
```

```python
import jax
import jax.numpy as jnp
from jax import lax
from jax.experimental import pallas as pl
from jax.experimental.pallas import tpu as pltpu
from jax.sharding import PartitionSpec as P


TILE = 128
SMALL = 4 * 1024 * 1024
PARAMS = pltpu.CompilerParams(vmem_limit_bytes=8 * 1024 * 1024)


def lookup(table, rows, cols):
    tiles = jnp.arange(table.shape[0], dtype=jnp.int32)
    row_pick = (rows[:, None] // TILE == tiles[None, :]).astype(jnp.bfloat16)
    col_pick = (tiles[:, None] == cols[None, :] // TILE).astype(jnp.bfloat16)
    left = jnp.dot(row_pick, table.astype(jnp.bfloat16))
    return jnp.dot(left, col_pick)


def span(start, count):
    return jnp.arange(count, dtype=jnp.int32) + start


def gathered(density, occupancy, square_filter, cube_filter):
    b, w = density.shape
    rows = span(lax.axis_index("rows") * b, b)
    cols = span(lax.axis_index("cols") * w, w)
    occupied = density * lookup(occupancy, rows, cols).astype(density.dtype)
    panel = lax.all_gather(occupied, "cols", axis=1, tiled=True)
    column = lax.all_gather(occupied, "rows", axis=0, tiled=True)
    total = jnp.dot(panel, column, preferred_element_type=jnp.float32)
    square = jnp.where(lookup(square_filter, rows, cols) > 0.5, total, 0.0).astype(jnp.bfloat16)
    square_rows = lax.all_gather(square, "cols", axis=1, tiled=True)
    cube = jnp.dot(square_rows, column, preferred_element_type=jnp.float32)
    cube = jnp.where(lookup(cube_filter, rows, cols) > 0.5, cube, 0.0)
    return 3.0 * square.astype(jnp.float32) - 2.0 * cube


def call(kernel, outs, args):
    held = [pltpu.with_memory_space_constraint(x, pltpu.VMEM) for x in args]
    spec = pl.BlockSpec(memory_space=pltpu.VMEM)
    return pl.pallas_call(
        kernel,
        out_shape=outs,
        in_specs=[spec] * len(held),
        out_specs=jax.tree.map(lambda _: spec, outs),
        compiler_params=PARAMS,
    )(*held)


def panel_kernel(*refs):
    pieces, (stored, panel) = refs[:-2], refs[-2:]
    panel[...] = jnp.concatenate([ref[...] for ref in pieces], axis=1) * stored[...]


def part_kernel(*refs):
    panels, (other, keep, cube_keep, pick, mine, yours) = refs[:-6], refs[-6:]
    b, w = mine.shape
    right = jnp.concatenate([ref[...] for ref in panels], axis=0)
    left = jnp.concatenate([panels[0][...], other[...]], axis=0)
    total = lax.dot_general(left, right, (((1,), (1,)), ((), ())), preferred_element_type=jnp.float32)
    square = (total * keep[...]).astype(jnp.bfloat16)
    cube = jnp.dot(square, right[:, :w], preferred_element_type=jnp.float32)
    own = jnp.dot(square, pick[...], preferred_element_type=jnp.float32)
    part = 3.0 * own - 2.0 * cube * cube_keep[...]
    mine[...] = part[:b]
    yours[...] = part[b:]


def turns(n):
    return sorted(range(1, n), key=lambda s: (s == 1, s))


def flips(n_rows):
    far = sorted(range(2, n_rows, 2), key=lambda f: (-f.bit_count(), f))
    return far + [1]


def permuted(density, occupancy, square_filter, cube_filter):
    b, w = density.shape
    n_rows, n = lax.axis_size("rows"), lax.axis_size("cols")
    r, j = lax.axis_index("rows"), lax.axis_index("cols")

    def swap(x, axis, flip):
        return lax.ppermute(x, axis, [(d, d ^ flip) for d in range(lax.axis_size(axis))])

    shifts = turns(n)
    pieces = [density] + [swap(density, "cols", s) for s in shifts]
    order = jnp.concatenate([span((j ^ s) * w, w) for s in [0] + shifts])
    rows = span(r * b, b)
    stored = lookup(occupancy, rows, order).astype(jnp.bfloat16)
    panel = call(panel_kernel, pltpu.VMEM((b, n * w), density.dtype), [*pieces, stored])

    got = {f: swap(panel, "rows", f) for f in flips(n_rows)}
    other = got.pop(1)
    kept = jnp.concatenate([span((r ^ f) * b, b) for f in [0] + list(got)])
    pair = jnp.concatenate([rows, span((r ^ 1) * b, b)])
    cols = span(j * w, w)
    keep = lookup(square_filter, pair, kept)
    cube_keep = lookup(cube_filter, pair, cols)
    pick = (kept[:, None] == cols[None, :]).astype(jnp.bfloat16)
    part = pltpu.VMEM((b, w), jnp.float32)
    args = [panel, *got.values(), other, keep, cube_keep, pick]
    mine, yours = call(part_kernel, [part, part], args)
    return mine + swap(yours, "rows", 1)


def solution(mesh):
    n_rows, n_cols = mesh.shape["rows"], mesh.shape["cols"]

    def on_device(density, *tables):
        powers = all(k & (k - 1) == 0 for k in (n_rows, n_cols))
        small = density.size * n_rows * n_cols * density.dtype.itemsize <= SMALL
        fits = small and powers and n_rows > 1 and density.shape[0] % 16 == 0
        return (permuted if fits else gathered)(density, *tables)

    placed = (P("rows", "cols"), P(), P(), P())
    return jax.shard_map(
        on_device, mesh=mesh, in_specs=placed, out_specs=P("rows", "cols"), check_vma=False
    )
```

```python
import functools

import jax
import jax.numpy as jnp
from jax import lax
from jax.experimental import pallas as pl
from jax.experimental.pallas import tpu as pltpu
from jax.sharding import PartitionSpec as P


TILE = 128
SMALL = 4 * 1024 * 1024
PARAMS = pltpu.CompilerParams(vmem_limit_bytes=8 * 1024 * 1024)


def lookup(table, rows, cols):
    tiles = jnp.arange(table.shape[0], dtype=jnp.int32)
    row_pick = (rows[:, None] // TILE == tiles[None, :]).astype(jnp.bfloat16)
    col_pick = (tiles[:, None] == cols[None, :] // TILE).astype(jnp.bfloat16)
    left = jnp.dot(row_pick, table.astype(jnp.bfloat16))
    return jnp.dot(left, col_pick)


def span(start, count):
    return jnp.arange(count, dtype=jnp.int32) + start


def gathered(density, occupancy, square_filter, cube_filter):
    b, w = density.shape
    rows = span(lax.axis_index("rows") * b, b)
    cols = span(lax.axis_index("cols") * w, w)
    occupied = density * lookup(occupancy, rows, cols).astype(density.dtype)
    panel = lax.all_gather(occupied, "cols", axis=1, tiled=True)
    column = lax.all_gather(occupied, "rows", axis=0, tiled=True)
    total = jnp.dot(panel, column, preferred_element_type=jnp.float32)
    square = jnp.where(lookup(square_filter, rows, cols) > 0.5, total, 0.0).astype(jnp.bfloat16)
    square_rows = lax.all_gather(square, "cols", axis=1, tiled=True)
    cube = jnp.dot(square_rows, column, preferred_element_type=jnp.float32)
    cube = jnp.where(lookup(cube_filter, rows, cols) > 0.5, cube, 0.0)
    return 3.0 * square.astype(jnp.float32) - 2.0 * cube


def call(kernel, outs, args, scratch=()):
    held = [pltpu.with_memory_space_constraint(x, pltpu.VMEM) for x in args]
    spec = pl.BlockSpec(memory_space=pltpu.VMEM)
    return pl.pallas_call(
        kernel,
        out_shape=outs,
        in_specs=[spec] * len(held),
        out_specs=jax.tree.map(lambda _: spec, outs),
        scratch_shapes=scratch,
        compiler_params=PARAMS,
    )(*held)


def group_turn():
    return (lax.axis_index("rows") // 2) ^ lax.axis_index("cols")


def nt(a, b):
    return lax.dot_general(a, b, (((1,), (1,)), ((), ())), preferred_element_type=jnp.float32)


def without(store, skip):
    n = store.shape[0]
    return jnp.concatenate([store[p + (skip <= p).astype(jnp.int32)] for p in range(n - 1)], axis=1)


def panel_kernel(*refs, shifts, ways):
    n = len(shifts)
    pieces, stored, panel, messages, store = refs[:n], refs[n], refs[n + 1], refs[n + 2 : -1], refs[-1]
    w = pieces[0].shape[1]
    keep = stored[...]
    for p, s in enumerate(shifts):
        store[s] = pieces[p][...] * keep[:, p * w : (p + 1) * w]
    turn = group_turn()
    for f, message in zip(ways, messages):
        message[...] = without(store, turn ^ (f // 2))
    panel[...] = jnp.concatenate([store[s] for s in range(n)], axis=1)


def finish(square, right, pick, cube_keep):
    cube = jnp.dot(square, right, preferred_element_type=jnp.float32)
    own = jnp.dot(square, pick[...], preferred_element_type=jnp.float32)
    return 3.0 * own - 2.0 * jnp.where(cube_keep[...] > 0, cube, 0.0)


def prep_kernel(panel, other, keep, cube_keep, pick, part, left_out, total, known_out, store, *, ways):
    n, _, w = store.shape
    b = panel.shape[0]
    mine, theirs = panel[...], other[...]
    left = jnp.concatenate([mine, theirs], axis=0)
    even = lax.axis_index("rows") % 2 == 1
    turn = group_turn()
    for q in range(n):
        store[q] = left[:, q * w : (q + 1) * w]
    left_out[...] = without(store, turn)
    known = []
    for f in ways:
        block = store[turn ^ (f // 2)]
        half = jnp.where(even, block[:, b:], block[:, :b])
        known.append(jnp.where(even, half, jnp.concatenate([half[b:], half[:b]], axis=0)))
    known = jnp.concatenate(known, axis=1)
    total[...] = jnp.dot(store[turn], known, preferred_element_type=jnp.float32)
    known_out[...] = known.astype(jnp.float32).T.astype(jnp.bfloat16)
    square = jnp.where(keep[...] > 0, nt(left, mine), 0.0).astype(jnp.bfloat16)
    part[...] = finish(square, mine[:, :w], pick, cube_keep)


def part_kernel(part, left, total, known, keep, cube_keep, pick, *refs):
    messages, (mine, yours) = refs[:-2], refs[-2:]
    b, w = mine.shape
    rows = jnp.concatenate([x[...] for x in messages], axis=0)
    square = jnp.where(keep[...] > 0, nt(left[...], rows) + total[...], 0.0).astype(jnp.bfloat16)
    right = jnp.where(group_turn() == 0, known[...], rows[:, :w])
    out = part[...] + finish(square, right, pick, cube_keep)
    mine[...] = out[:b]
    yours[...] = out[b:]


def turns(n):
    return [n - 1] + list(range(1, n - 1)) + [0]


def flips(n_rows):
    return list(range(n_rows - 1, 0, -2))


def permuted(density, occupancy, square_filter, cube_filter):
    b, w = density.shape
    n_rows, n = lax.axis_size("rows"), lax.axis_size("cols")
    j = lax.axis_index("cols")
    me = lax.axis_index("rows") ^ 1

    def swap(x, row_flip, col_flip):
        pairs = [(p * n + q, (p ^ row_flip) * n + (q ^ col_flip)) for p in range(n_rows) for q in range(n)]
        return lax.ppermute(x, ("rows", "cols"), pairs)

    shifts = turns(n)
    pieces = [swap(density, 1, s) for s in shifts]
    order = jnp.concatenate([span((j ^ s) * w, w) for s in shifts])
    rows = span(me * b, b)
    stored = lookup(occupancy, rows, order).astype(jnp.bfloat16)

    far = flips(n_rows)[:-1]
    held = lambda h, k, dtype=jnp.bfloat16: pltpu.VMEM((h, k), dtype)
    outs = [held(b, n * w)] + [held(b, (n - 1) * w)] * len(far)
    kernel = functools.partial(panel_kernel, shifts=shifts, ways=far)
    panel, *messages = call(kernel, outs, [*pieces, stored], [pltpu.VMEM((n, b, w), density.dtype)])
    got = [swap(x, f, 0) for f, x in zip(far, messages)]
    other = swap(panel, 1, 0)

    panel, square_filter, cube_filter = lax.optimization_barrier((panel, square_filter, cube_filter))
    kept = jnp.concatenate([span((me ^ f) * b, b) for f in far])
    pair = jnp.concatenate([rows, span((me ^ 1) * b, b)])
    cols = span(j * w, w)
    cube_keep = lookup(cube_filter, pair, cols)
    pick = lambda x: (x[:, None] == cols[None, :]).astype(jnp.bfloat16)
    height, width = 2 * b, len(far) * b
    outs = [held(height, w, jnp.float32), held(height, (n - 1) * w), held(height, width, jnp.float32), held(width, w)]
    args = [panel, other, lookup(square_filter, pair, rows), cube_keep, pick(rows)]
    store = [pltpu.VMEM((n, height, w), density.dtype)]
    ready = call(functools.partial(prep_kernel, ways=far), outs, args, store)
    args = [*ready, lookup(square_filter, pair, kept), cube_keep, pick(kept), *got]
    ends = [held(b, w, jnp.float32)] * 2
    mine, yours = call(part_kernel, ends, args)
    return yours + swap(mine, 1, 0)


def solution(mesh):
    n_rows, n_cols = mesh.shape["rows"], mesh.shape["cols"]

    def on_device(density, *tables):
        powers = all(k & (k - 1) == 0 for k in (n_rows, n_cols))
        small = density.size * n_rows * n_cols * density.dtype.itemsize <= SMALL
        b, w = density.shape
        fits = small and powers and n_rows == 2 * n_cols and w == 2 * b and b % 16 == 0
        return (permuted if fits else gathered)(density, *tables)

    placed = (P("rows", "cols"), P(), P(), P())
    return jax.shard_map(
        on_device, mesh=mesh, in_specs=placed, out_specs=P("rows", "cols"), check_vma=False
    )
```

```python
import functools

import jax
import jax.numpy as jnp
from jax import lax
from jax.experimental import pallas as pl
from jax.experimental.pallas import tpu as pltpu
from jax.sharding import PartitionSpec as P


TILE = 128
SMALL = 4 * 1024 * 1024
PARAMS = pltpu.CompilerParams(vmem_limit_bytes=8 * 1024 * 1024)


def lookup(table, rows, cols):
    tiles = jnp.arange(table.shape[0], dtype=jnp.int32)
    row_pick = (rows[:, None] // TILE == tiles[None, :]).astype(jnp.bfloat16)
    col_pick = (tiles[:, None] == cols[None, :] // TILE).astype(jnp.bfloat16)
    left = jnp.dot(row_pick, table.astype(jnp.bfloat16))
    return jnp.dot(left, col_pick)


def span(start, count):
    return jnp.arange(count, dtype=jnp.int32) + start


def gathered(density, occupancy, square_filter, cube_filter):
    b, w = density.shape
    rows = span(lax.axis_index("rows") * b, b)
    cols = span(lax.axis_index("cols") * w, w)
    occupied = density * lookup(occupancy, rows, cols).astype(density.dtype)
    panel = lax.all_gather(occupied, "cols", axis=1, tiled=True)
    column = lax.all_gather(occupied, "rows", axis=0, tiled=True)
    total = jnp.dot(panel, column, preferred_element_type=jnp.float32)
    square = jnp.where(lookup(square_filter, rows, cols) > 0.5, total, 0.0).astype(jnp.bfloat16)
    square_rows = lax.all_gather(square, "cols", axis=1, tiled=True)
    cube = jnp.dot(square_rows, column, preferred_element_type=jnp.float32)
    cube = jnp.where(lookup(cube_filter, rows, cols) > 0.5, cube, 0.0)
    return 3.0 * square.astype(jnp.float32) - 2.0 * cube


def call(kernel, outs, args, scratch=()):
    held = [pltpu.with_memory_space_constraint(x, pltpu.VMEM) for x in args]
    spec = pl.BlockSpec(memory_space=pltpu.VMEM)
    return pl.pallas_call(
        kernel,
        out_shape=outs,
        in_specs=[spec] * len(held),
        out_specs=jax.tree.map(lambda _: spec, outs),
        scratch_shapes=scratch,
        compiler_params=PARAMS,
    )(*held)


def group_turn():
    return (lax.axis_index("rows") // 2) ^ lax.axis_index("cols")


def nt(a, b):
    return lax.dot_general(a, b, (((1,), (1,)), ((), ())), preferred_element_type=jnp.float32)


def without(store, skip):
    n = store.shape[0]
    return jnp.concatenate([store[p + (skip <= p).astype(jnp.int32)] for p in range(n - 1)], axis=1)


def panel_kernel(*refs, shifts, ways):
    n = len(shifts)
    pieces, stored, panel, messages = dict(zip(shifts, refs)), refs[n], refs[n + 1], refs[n + 2 :]
    w = pieces[0].shape[1]
    whole = jnp.concatenate([pieces[s][...] for s in range(n)], axis=1) * stored[...]
    panel[...] = whole
    ahead, behind = whole[:, : (n - 1) * w], whole[:, w:]
    lane = lax.broadcasted_iota(jnp.int32, ahead.shape, 1)
    turn = group_turn()
    for f, message in zip(ways, messages):
        message[...] = jnp.where(lane < (turn ^ (f // 2)) * w, ahead, behind)


def finish(square, right, pick, cube_keep):
    cube = jnp.dot(square, right, preferred_element_type=jnp.float32)
    own = jnp.dot(square, pick[...], preferred_element_type=jnp.float32)
    return 3.0 * own - 2.0 * jnp.where(cube_keep[...] > 0, cube, 0.0)


def prep_kernel(panel, other, keep, cube_keep, pick, part, left_out, total, known_out, store, *, ways):
    n, _, w = store.shape
    b = panel.shape[0]
    mine, theirs = panel[...], other[...]
    left = jnp.concatenate([mine, theirs], axis=0)
    even = lax.axis_index("rows") % 2 == 1
    turn = group_turn()
    for q in range(n):
        store[q] = left[:, q * w : (q + 1) * w]
    left_out[...] = without(store, turn)
    known = []
    for f in ways:
        block = store[turn ^ (f // 2)]
        half = jnp.where(even, block[:, b:], block[:, :b])
        known.append(jnp.where(even, half, jnp.concatenate([half[b:], half[:b]], axis=0)))
    known = jnp.concatenate(known, axis=1)
    total[...] = jnp.dot(store[turn], known, preferred_element_type=jnp.float32)
    known_out[...] = known.astype(jnp.float32).T.astype(jnp.bfloat16)
    square = jnp.where(keep[...] > 0, nt(left, mine), 0.0).astype(jnp.bfloat16)
    part[...] = finish(square, mine[:, :w], pick, cube_keep)


def part_kernel(part, left, total, known, keep, cube_keep, pick, *refs):
    messages, (mine, yours) = refs[:-2], refs[-2:]
    b, w = mine.shape
    rows = jnp.concatenate([x[...] for x in messages], axis=0)
    square = jnp.where(keep[...] > 0, nt(left[...], rows) + total[...], 0.0).astype(jnp.bfloat16)
    right = jnp.where(group_turn() == 0, known[...], rows[:, :w])
    out = part[...] + finish(square, right, pick, cube_keep)
    mine[...] = out[:b]
    yours[...] = out[b:]


def turns(n):
    return [n - 1] + list(range(1, n - 1)) + [0]


def flips(n_rows):
    return list(range(n_rows - 1, 0, -2))


def permuted(density, occupancy, square_filter, cube_filter):
    b, w = density.shape
    n_rows, n = lax.axis_size("rows"), lax.axis_size("cols")
    j = lax.axis_index("cols")
    me = lax.axis_index("rows") ^ 1

    def swap(x, row_flip, col_flip):
        pairs = [(p * n + q, (p ^ row_flip) * n + (q ^ col_flip)) for p in range(n_rows) for q in range(n)]
        return lax.ppermute(x, ("rows", "cols"), pairs)

    shifts = turns(n)
    pieces = [swap(density, 1, s) for s in shifts]
    order = jnp.concatenate([span((j ^ s) * w, w) for s in range(n)])
    rows = span(me * b, b)
    stored = lookup(occupancy, rows, order).astype(jnp.bfloat16)

    far = flips(n_rows)[:-1]
    held = lambda h, k, dtype=jnp.bfloat16: pltpu.VMEM((h, k), dtype)
    outs = [held(b, n * w)] + [held(b, (n - 1) * w)] * len(far)
    kernel = functools.partial(panel_kernel, shifts=shifts, ways=far)
    panel, *messages = call(kernel, outs, [*pieces, stored])
    got = [swap(x, f, 0) for f, x in zip(far, messages)]
    other = swap(panel, 1, 0)

    panel, square_filter, cube_filter = lax.optimization_barrier((panel, square_filter, cube_filter))
    kept = jnp.concatenate([span((me ^ f) * b, b) for f in far])
    pair = jnp.concatenate([rows, span((me ^ 1) * b, b)])
    cols = span(j * w, w)
    cube_keep = lookup(cube_filter, pair, cols)
    pick = lambda x: (x[:, None] == cols[None, :]).astype(jnp.bfloat16)
    height, width = 2 * b, len(far) * b
    outs = [held(height, w, jnp.float32), held(height, (n - 1) * w), held(height, width, jnp.float32), held(width, w)]
    args = [panel, other, lookup(square_filter, pair, rows), cube_keep, pick(rows)]
    store = [pltpu.VMEM((n, height, w), density.dtype)]
    ready = call(functools.partial(prep_kernel, ways=far), outs, args, store)
    args = [*ready, lookup(square_filter, pair, kept), cube_keep, pick(kept), *got]
    ends = [held(b, w, jnp.float32)] * 2
    mine, yours = call(part_kernel, ends, args)
    return yours + swap(mine, 1, 0)


def solution(mesh):
    n_rows, n_cols = mesh.shape["rows"], mesh.shape["cols"]

    def on_device(density, *tables):
        powers = all(k & (k - 1) == 0 for k in (n_rows, n_cols))
        small = density.size * n_rows * n_cols * density.dtype.itemsize <= SMALL
        b, w = density.shape
        fits = small and powers and n_rows == 2 * n_cols and w == 2 * b and b % 16 == 0
        return (permuted if fits else gathered)(density, *tables)

    placed = (P("rows", "cols"), P(), P(), P())
    return jax.shard_map(
        on_device, mesh=mesh, in_specs=placed, out_specs=P("rows", "cols"), check_vma=False
    )
```

```python
import functools

import jax
import jax.numpy as jnp
from jax import lax
from jax.experimental import pallas as pl
from jax.experimental.pallas import tpu as pltpu
from jax.sharding import PartitionSpec as P


TILE = 128
SMALL = 4 * 1024 * 1024
PARAMS = pltpu.CompilerParams(vmem_limit_bytes=8 * 1024 * 1024)


def lookup(table, rows, cols):
    tiles = jnp.arange(table.shape[0], dtype=jnp.int32)
    row_pick = (rows[:, None] // TILE == tiles[None, :]).astype(jnp.bfloat16)
    col_pick = (tiles[:, None] == cols[None, :] // TILE).astype(jnp.bfloat16)
    left = jnp.dot(row_pick, table.astype(jnp.bfloat16))
    return jnp.dot(left, col_pick)


def span(start, count):
    return jnp.arange(count, dtype=jnp.int32) + start


def gathered(density, occupancy, square_filter, cube_filter):
    b, w = density.shape
    rows = span(lax.axis_index("rows") * b, b)
    cols = span(lax.axis_index("cols") * w, w)
    occupied = density * lookup(occupancy, rows, cols).astype(density.dtype)
    panel = lax.all_gather(occupied, "cols", axis=1, tiled=True)
    column = lax.all_gather(occupied, "rows", axis=0, tiled=True)
    total = jnp.dot(panel, column, preferred_element_type=jnp.float32)
    square = jnp.where(lookup(square_filter, rows, cols) > 0.5, total, 0.0).astype(jnp.bfloat16)
    square_rows = lax.all_gather(square, "cols", axis=1, tiled=True)
    cube = jnp.dot(square_rows, column, preferred_element_type=jnp.float32)
    cube = jnp.where(lookup(cube_filter, rows, cols) > 0.5, cube, 0.0)
    return 3.0 * square.astype(jnp.float32) - 2.0 * cube


def call(kernel, outs, args, scratch=()):
    held = [pltpu.with_memory_space_constraint(x, pltpu.VMEM) for x in args]
    spec = pl.BlockSpec(memory_space=pltpu.VMEM)
    return pl.pallas_call(
        kernel,
        out_shape=outs,
        in_specs=[spec] * len(held),
        out_specs=jax.tree.map(lambda _: spec, outs),
        scratch_shapes=scratch,
        compiler_params=PARAMS,
    )(*held)


def group_turn():
    return (lax.axis_index("rows") // 2) ^ lax.axis_index("cols")


def nt(a, b):
    return lax.dot_general(a, b, (((1,), (1,)), ((), ())), preferred_element_type=jnp.float32)


def without(store, skip):
    n = store.shape[0]
    return jnp.concatenate([store[p + (skip <= p).astype(jnp.int32)] for p in range(n - 1)], axis=1)


def panel_kernel(*refs, shifts, ways):
    n = len(shifts)
    pieces, stored, panel, messages = dict(zip(shifts, refs)), refs[n], refs[n + 1], refs[n + 2 :]
    w = pieces[0].shape[1]
    whole = jnp.concatenate([pieces[s][...] for s in range(n)], axis=1) * stored[...]
    panel[...] = whole
    ahead, behind = whole[:, : (n - 1) * w], whole[:, w:]
    lane = lax.broadcasted_iota(jnp.int32, ahead.shape, 1)
    turn = group_turn()
    for f, message in zip(ways, messages):
        message[...] = jnp.where(lane < (turn ^ (f // 2)) * w, ahead, behind)


def finish(square, right, pick, cube_keep):
    cube = jnp.dot(square, right, preferred_element_type=jnp.float32)
    own = jnp.dot(square, pick[...], preferred_element_type=jnp.float32)
    return 3.0 * own - 2.0 * jnp.where(cube_keep[...] > 0, cube, 0.0)


def prep_kernel(panel, other, keep, cube_keep, pick, part, left_out, total, known_out, store, *, ways):
    n, _, w = store.shape
    b = panel.shape[0]
    mine, theirs = panel[...], other[...]
    left = jnp.concatenate([mine, theirs], axis=0)
    even = lax.axis_index("rows") % 2 == 1
    turn = group_turn()
    for q in range(n):
        store[q] = left[:, q * w : (q + 1) * w]
    left_out[...] = without(store, turn)
    known = []
    for f in ways:
        block = store[turn ^ (f // 2)]
        half = jnp.where(even, block[:, b:], block[:, :b])
        known.append(jnp.where(even, half, jnp.concatenate([half[b:], half[:b]], axis=0)))
    known = jnp.concatenate(known, axis=1)
    total[...] = jnp.dot(store[turn], known, preferred_element_type=jnp.float32)
    known_out[...] = known.astype(jnp.float32).T.astype(jnp.bfloat16)
    square = jnp.where(keep[...] > 0, nt(left, mine), 0.0).astype(jnp.bfloat16)
    part[...] = finish(square, mine[:, :w], pick, cube_keep)


def part_kernel(part, left, total, known, keep, cube_keep, pick, *refs):
    messages, (mine, yours) = refs[:-2], refs[-2:]
    b, w = mine.shape
    rows = jnp.concatenate([x[...] for x in messages], axis=0)
    squares = []
    for k in range(2):
        at = slice(k * b, (k + 1) * b)
        product = nt(left[at, :], rows) + total[at, :]
        squares.append(jnp.where(keep[at, :] > 0, product, 0.0).astype(jnp.bfloat16))
    square = jnp.concatenate(squares, axis=0)
    right = jnp.where(group_turn() == 0, known[...], rows[:, :w])
    out = part[...] + finish(square, right, pick, cube_keep)
    mine[...] = out[:b]
    yours[...] = out[b:]


def turns(n):
    return [n - 1] + list(range(1, n - 1)) + [0]


def flips(n_rows):
    return list(range(n_rows - 1, 0, -2))


def add_kernel(a, b, out, store, done):
    h = out.shape[0] // 2
    copies = [pltpu.make_async_copy(store.at[pl.ds(k * h, h)], out.at[pl.ds(k * h, h)], done.at[k]) for k in range(2)]
    for k, copy in enumerate(copies):
        at = pl.ds(k * h, h)
        store[at, :] = a[at, :] + b[at, :]
        copy.start()
    for copy in copies:
        copy.wait()


def add(a, b):
    held = [pltpu.with_memory_space_constraint(x, pltpu.VMEM) for x in (a, b)]
    spec = pl.BlockSpec(memory_space=pltpu.VMEM)
    return pl.pallas_call(
        add_kernel,
        out_shape=jax.ShapeDtypeStruct(a.shape, a.dtype),
        in_specs=[spec] * 2,
        out_specs=pl.BlockSpec(memory_space=pl.ANY),
        scratch_shapes=[pltpu.VMEM(a.shape, a.dtype), pltpu.SemaphoreType.DMA((2,))],
        compiler_params=PARAMS,
        name="add",
    )(*held)


def permuted(density, occupancy, square_filter, cube_filter):
    b, w = density.shape
    n_rows, n = lax.axis_size("rows"), lax.axis_size("cols")
    j = lax.axis_index("cols")
    me = lax.axis_index("rows") ^ 1

    def swap(x, row_flip, col_flip):
        pairs = [(p * n + q, (p ^ row_flip) * n + (q ^ col_flip)) for p in range(n_rows) for q in range(n)]
        return lax.ppermute(x, ("rows", "cols"), pairs)

    shifts = turns(n)
    pieces = [swap(density, 1, s) for s in shifts]
    order = jnp.concatenate([span((j ^ s) * w, w) for s in range(n)])
    rows = span(me * b, b)
    stored = lookup(occupancy, rows, order).astype(jnp.bfloat16)

    far = flips(n_rows)[:-1]
    held = lambda h, k, dtype=jnp.bfloat16: pltpu.VMEM((h, k), dtype)
    outs = [held(b, n * w)] + [held(b, (n - 1) * w)] * len(far)
    kernel = functools.partial(panel_kernel, shifts=shifts, ways=far)
    panel, *messages = call(kernel, outs, [*pieces, stored])
    got = [swap(x, f, 0) for f, x in zip(far, messages)]
    other = swap(panel, 1, 0)

    panel, square_filter, cube_filter = lax.optimization_barrier((panel, square_filter, cube_filter))
    kept = jnp.concatenate([span((me ^ f) * b, b) for f in far])
    pair = jnp.concatenate([rows, span((me ^ 1) * b, b)])
    cols = span(j * w, w)
    cube_keep = lookup(cube_filter, pair, cols)
    pick = lambda x: (x[:, None] == cols[None, :]).astype(jnp.bfloat16)
    height, width = 2 * b, len(far) * b
    outs = [held(height, w, jnp.float32), held(height, (n - 1) * w), held(height, width, jnp.float32), held(width, w)]
    args = [panel, other, lookup(square_filter, pair, rows), cube_keep, pick(rows)]
    store = [pltpu.VMEM((n, height, w), density.dtype)]
    ready = call(functools.partial(prep_kernel, ways=far), outs, args, store)
    args = [*ready, lookup(square_filter, pair, kept), cube_keep, pick(kept), *got]
    ends = [held(b, w, jnp.float32)] * 2
    mine, yours = call(part_kernel, ends, args)
    return add(yours, swap(mine, 1, 0))


def solution(mesh):
    n_rows, n_cols = mesh.shape["rows"], mesh.shape["cols"]

    def on_device(density, *tables):
        powers = all(k & (k - 1) == 0 for k in (n_rows, n_cols))
        small = density.size * n_rows * n_cols * density.dtype.itemsize <= SMALL
        b, w = density.shape
        fits = small and powers and n_rows == 2 * n_cols and w == 2 * b and b % 16 == 0
        return (permuted if fits else gathered)(density, *tables)

    placed = (P("rows", "cols"), P(), P(), P())
    return jax.shard_map(
        on_device, mesh=mesh, in_specs=placed, out_specs=P("rows", "cols"), check_vma=False
    )
```
